8 devices in a mesh: stage: 1 (over z), fsdp: 2 (over y), tp: 4 (over x, core).
Axes of the slice: x: 2, y: 2, z: 1, core: 2. Of those that a mesh axis runs over, the one named last changes fastest.
Arguments:
- weight: float32 [1, 11008, 4096], P('stage', 'fsdp', 'tp')
- momentum: float32 [1, 11008, 4096], P('stage', 'fsdp', 'tp')
- gradient: bfloat16 [1, 11008, 4096], P('stage', 'fsdp', 'tp')
- learn_rate: float32 [], replicated
- mom_coef: float32 [], replicated
- weight_decay: float32 [], replicated
Outputs:
- output 1: float32 [1, 11008, 4096], P('stage', 'fsdp', 'tp')
- output 2: float32 [1, 11008, 4096], P('stage', 'fsdp', 'tp')
All inputs are finite; a program needn't handle non-finite values.
Results may differ from the reference program's by a relative error of at most 0.00931572.
Values are sent between devices in bfloat16 or wider.
A program may use at most 1 GiB of HBM per device.

```python
import jax
import jax.numpy as jnp
from jax import lax
import math

MATRICES = 1
ROW_DIM = 11008
COL_DIM = 4096
NS_STEPS = 5

COEF_A = 3.4445
COEF_B = -4.7750
COEF_C = 2.0315
NORM_EPS = 1e-7


def low_rank_draw(key, rank_dim):
    key_u, key_v, key_n = jax.random.split(key, 3)
    decay = jnp.exp(-0.35 * jnp.arange(rank_dim, dtype=jnp.float32))
    decay = decay / jnp.sqrt(jnp.mean(decay * decay))
    left = jax.random.normal(key_u, (MATRICES, ROW_DIM, rank_dim), jnp.float32) * decay
    right = jax.random.normal(key_v, (MATRICES, rank_dim, COL_DIM), jnp.float32)
    noise = jax.random.normal(key_n, (MATRICES, ROW_DIM, COL_DIM), jnp.float32)
    low_part = jnp.einsum('erk,ekc->erc', left, right) / math.sqrt(rank_dim)
    return low_part + 0.5 * noise


def setup_inputs(seed: int = 0, part: int = 0) -> dict:
    base_key = jax.random.key(seed)
    part_key = jax.random.fold_in(base_key, part)
    key_w, key_m, key_g = jax.random.split(part_key, 3)
    shared_key = jax.random.key(seed + 4241)
    key_lr, key_mu, key_wd = jax.random.split(shared_key, 3)
    weight = 0.25 * jax.random.normal(key_w, (MATRICES, ROW_DIM, COL_DIM), jnp.float32)
    momentum = low_rank_draw(key_m, 8)
    gradient = low_rank_draw(key_g, 8).astype(jnp.bfloat16)
    learn_rate = jax.random.uniform(key_lr, (), jnp.float32, 0.5, 1.0)
    mom_coef = jax.random.uniform(key_mu, (), jnp.float32, 0.1, 0.95)
    weight_decay = jax.random.uniform(key_wd, (), jnp.float32, 0.2, 0.6)
    return {'weight': weight, 'momentum': momentum, 'gradient': gradient, 'learn_rate': learn_rate, 'mom_coef': mom_coef, 'weight_decay': weight_decay}


def newton_schulz(x_iter):
    for step_idx in range(NS_STEPS):
        gram_mat = jnp.dot(x_iter.T, x_iter, preferred_element_type=jnp.float32).astype(jnp.bfloat16)
        gram_sq = jnp.dot(gram_mat, gram_mat, preferred_element_type=jnp.float32).astype(jnp.bfloat16)
        poly_mat = (COEF_B * gram_mat.astype(jnp.float32) + COEF_C * gram_sq.astype(jnp.float32)).astype(jnp.bfloat16)
        update = jnp.dot(x_iter, poly_mat.T, preferred_element_type=jnp.float32)
        x_iter = (COEF_A * x_iter.astype(jnp.float32) + update).astype(jnp.bfloat16)
    return x_iter


def reference(weight, momentum, gradient, learn_rate, mom_coef, weight_decay):
    def one_matrix(blocks):
        w_mat, m_mat, g_mat = blocks
        grad_full = g_mat.astype(jnp.float32)
        mom_new = mom_coef * m_mat + grad_full
        nesterov = grad_full + mom_coef * mom_new
        norm_val = jnp.sqrt(jnp.sum(nesterov * nesterov))
        x_iter = (nesterov / (norm_val + NORM_EPS)).astype(jnp.bfloat16)
        x_iter = newton_schulz(x_iter)
        step_scale = learn_rate * 0.2 * math.sqrt(ROW_DIM)
        w_new = (1.0 - learn_rate * weight_decay) * w_mat - step_scale * x_iter.astype(jnp.float32)
        return w_new, mom_new
    new_weight, new_momentum = lax.map(one_matrix, (weight, momentum, gradient))
    return (new_weight, new_momentum)
```

```python
import functools
import math

import jax
import jax.numpy as jnp
from jax import lax
from jax.experimental import pallas as pl
from jax.experimental.pallas import tpu as pltpu
from jax.sharding import PartitionSpec as P


NS_STEPS = 5
COEF_A = 3.4445
COEF_B = -4.7750
COEF_C = 2.0315
NORM_EPS = 1e-7


BS = 512
VMEM_LIMIT = 58 * 1024 * 1024
BF16, F32 = jnp.bfloat16, jnp.float32
CORE, ZERO, XPOS, YPOS, KEEP, SEND, MINE, SEL = 8, 9, 10, 11, 12, 13, 14, 16


def call(kernel, grid, in_specs, out_specs, out_shape, idx, args, flops, nbytes, scratch=(), aliases=None):
    return pl.pallas_call(
        kernel,
        grid_spec=pltpu.PrefetchScalarGridSpec(
            num_scalar_prefetch=1, grid=grid, in_specs=in_specs, out_specs=out_specs, scratch_shapes=scratch
        ),
        out_shape=out_shape,
        input_output_aliases=aliases or {},
        compiler_params=pltpu.CompilerParams(
            vmem_limit_bytes=VMEM_LIMIT, dimension_semantics=('arbitrary',) * len(grid)
        ),
        cost_estimate=pl.CostEstimate(flops=flops, bytes_accessed=nbytes, transcendentals=0),
    )(idx, *args)


class Order:
    def __init__(self, idx):
        self.idx = idx

    def after(self, *arrays):
        self.idx = lax.optimization_barrier((self.idx,) + arrays)[0]


def start_kernel(mom_ref, grad_ref, scal_ref, out_ref):
    grad = grad_ref[...].astype(F32)
    nesterov = grad + scal_ref[0] * (scal_ref[0] * mom_ref[...] + grad)
    out_ref[...] = (nesterov / scal_ref[1]).astype(BF16).T


def start_x(momentum, gradient, scalars):
    rows, cols = momentum.shape
    spec = pl.BlockSpec((BS, cols), lambda i: (i, 0))
    return pl.pallas_call(
        start_kernel,
        name='start',
        grid=(pl.cdiv(rows, BS),),
        in_specs=[spec, spec, pl.BlockSpec(memory_space=pltpu.SMEM)],
        out_specs=pl.BlockSpec((cols, BS), lambda i: (0, i)),
        out_shape=jax.ShapeDtypeStruct((cols, rows), BF16),
        compiler_params=pltpu.CompilerParams(vmem_limit_bytes=VMEM_LIMIT, dimension_semantics=('arbitrary',)),
        cost_estimate=pl.CostEstimate(flops=rows * cols * 64, bytes_accessed=rows * cols * 8, transcendentals=0),
    )(momentum, gradient, scalars)


def gram_kernel(depth, tile, idx_ref, rows_ref, *refs):
    keep_ref, send_ref = refs[-2:]
    step = pl.program_id(0)
    n_steps = pl.cdiv(depth, tile)
    rest = depth - (n_steps - 1) * tile

    def product(width):
        lhs = jnp.concatenate([ref[0, :, :width] for ref in refs[:-2]], axis=0)
        acc = jnp.dot(lhs, rows_ref[0, :, :width].T, preferred_element_type=F32)
        half = acc.shape[0] // 2
        return acc[:half].reshape(keep_ref.shape), acc[half:].reshape(send_ref.shape)

    @pl.when(step == 0)
    def _():
        keep_ref[...], send_ref[...] = product(tile)

    @pl.when((step > 0) & (step < n_steps - 1))
    def _():
        keep, send = product(tile)
        keep_ref[...] += keep
        send_ref[...] += send

    @pl.when(step == n_steps - 1)
    def _():
        keep, send = product(rest)
        keep_ref[...] += keep
        send_ref[...] += send


def gram_unit(idx, pieces, q, p_lo, p_hi):
    num = 2 * (p_hi - p_lo)
    rows_arr, rows_at = pieces[2 * q]
    depth = rows_arr.shape[-1]
    tile = pl.cdiv(depth, 4 * 128) * 128
    in_specs = [pl.BlockSpec((1, BS, tile), lambda k, s: (s[rows_at], 0, k))]
    args = [rows_arr]
    for part in (KEEP, SEND):
        for arr, at in pieces[2 * p_lo:2 * p_hi]:
            in_specs.append(pl.BlockSpec((1, BS // 4, tile), lambda k, s, at=at, part=part: (s[at], s[part], k)))
            args.append(arr)
    out = jax.ShapeDtypeStruct((num, BS // 4, BS), F32)
    out_spec = pl.BlockSpec((num, BS // 4, BS), lambda k, s: (0, 0, 0))
    return call(
        functools.partial(gram_kernel, depth, tile), (pl.cdiv(depth, tile),),
        in_specs, (out_spec, out_spec), (out, out), idx, args,
        2 * num * (BS // 2) * BS * depth, (num + 2) * BS * depth,
    )


def square_kernel(idx_ref, rows_ref, cols_ref, own_ref, out_ref):
    acc = jnp.dot(rows_ref[...], cols_ref[...], preferred_element_type=F32)
    sq = acc.astype(BF16).astype(F32)
    out_ref[...] = (COEF_B * own_ref[...].astype(F32) + COEF_C * sq).astype(BF16)


def poly_rows(idx, gram, row_at):
    dim = gram.shape[0]
    num = dim // BS
    in_specs = [
        pl.BlockSpec((BS, dim), lambda i, s: (s[row_at], 0)),
        pl.BlockSpec((dim, BS), lambda i, s: (0, i)),
        pl.BlockSpec((BS, BS), lambda i, s: (s[row_at], i)),
    ]
    out_spec = pl.BlockSpec((BS, BS), lambda i, s: (0, jnp.bitwise_xor(i, s[CORE])))
    return call(
        square_kernel, (num,), in_specs, out_spec,
        jax.ShapeDtypeStruct((BS, dim), BF16), idx, [gram, gram, gram], 2 * BS * dim * dim, dim * dim * 2,
    )


def mix(b_ref, refs):
    acc = jnp.dot(b_ref[:, :BS], refs[0][0], preferred_element_type=F32)
    for pos in range(1, len(refs)):
        acc += jnp.dot(b_ref[:, pos * BS:(pos + 1) * BS], refs[pos][0], preferred_element_type=F32)
    return acc


def update_kernel(sel, idx_ref, b_ref, *refs):
    out_ref = refs[-1]
    acc = mix(b_ref, refs[:-1])
    out_ref[0] = (COEF_A * refs[sel][0].astype(F32) + acc).astype(BF16)


def piece_specs(pieces, tile):
    specs = [pl.BlockSpec((1, BS, tile), lambda i, s, at=at: (s[at], 0, i)) for _, at in pieces]
    return specs, [arr for arr, _ in pieces]


def update_chunk(idx, poly, pieces, q):
    num = len(pieces)
    depth = pieces[0][0].shape[-1]
    tile = BS
    specs, args = piece_specs(pieces, tile)
    return call(
        functools.partial(update_kernel, 2 * q), (pl.cdiv(depth, tile),),
        [pl.BlockSpec(poly.shape, lambda i, s: (0, 0))] + specs, pl.BlockSpec((1, BS, tile), lambda i, s: (0, 0, i)),
        jax.ShapeDtypeStruct((1, BS, depth), BF16), idx, [poly] + args,
        2 * BS * BS * num * depth, num * BS * depth * 2,
    )


def finish_kernel(half, num, idx_ref, scal_ref, b_ref, w_ref, *refs):
    old_ref = refs[-1]
    out_ref = refs[num]
    acc = mix(b_ref, refs[:num])
    for pos in range(num):
        @pl.when(idx_ref[SEL + half] == pos)
        def _(pos=pos):
            old_ref[...] = refs[pos][0]
    x_last = (COEF_A * old_ref[...].astype(F32) + acc).astype(BF16).T
    out_ref[...] = scal_ref[0] * w_ref[...] - scal_ref[1] * x_last.astype(F32)


def finish(idx, scalars, poly, weight, pieces, half, before):
    num = len(pieces)
    rows = weight.shape[0]
    tile = BS
    specs, args = piece_specs(pieces, tile)
    w_spec = pl.BlockSpec((tile, BS), lambda i, s: (i, half))
    in_specs = [pl.BlockSpec(memory_space=pltpu.SMEM), pl.BlockSpec(poly.shape, lambda i, s: (0, 0)), w_spec] + specs
    args = [scalars, poly, weight] + args
    kernel = functools.partial(finish_kernel, half, num)
    aliases = None
    if before is not None:
        in_specs.append(pl.BlockSpec(memory_space=pl.ANY))
        args.append(before)
        aliases = {len(args): 0}
        body = kernel

        def kernel(*refs):
            body(*refs[:4 + num], *refs[5 + num:])
    return call(
        kernel, (pl.cdiv(rows, tile),), in_specs, w_spec,
        jax.ShapeDtypeStruct(weight.shape, F32), idx, args,
        2 * BS * BS * num * rows, num * BS * rows * 2, scratch=[pltpu.VMEM((BS, tile), BF16)], aliases=aliases,
    )


def unpack_kernel(n_direct, idx_ref, *refs):
    out_ref = refs[-1]
    step = pl.program_id(0)
    core, x_pos, y_pos = idx_ref[CORE], idx_ref[XPOS], idx_ref[YPOS]
    rows = BS // 4

    def place(mirror):
        for side in range(2):
            src = jnp.bitwise_xor(core, side)
            line = pl.ds(pl.multiple_of(src * BS, BS), BS)
            for k in range(4):
                off = jnp.bitwise_xor(x_pos, k // 2) * (2 * rows) + jnp.bitwise_xor(y_pos, k % 2) * rows
                for h in range(2):
                    spot = pl.ds(pl.multiple_of(jnp.bitwise_xor(src, h) * BS + off, rows), rows)
                    if mirror:
                        out_ref[line, spot] = refs[4 * side + k][h].T
                    else:
                        out_ref[spot, line] = refs[4 * side + k][h]

    @pl.when(step < n_direct)
    def _():
        place(False)

    @pl.when(step >= n_direct)
    def _():
        place(True)


def unpack(idx, gram, parts, dim, q, p_lo, p_hi):
    n_direct = p_hi - p_lo
    n_mirror = min(p_hi, q) - p_lo

    def in_map(t, s):
        return jnp.where(t < n_direct, t, t - n_direct), 0, 0

    def out_map(t, s):
        direct = t < n_direct
        return jnp.where(direct, p_lo + t, q), jnp.where(direct, q, p_lo + t - n_direct)

    in_specs = [pl.BlockSpec((2, BS // 4, BS), in_map) for _ in parts]
    args = list(parts)
    kernel = functools.partial(unpack_kernel, n_direct)
    aliases = None
    if gram is not None:
        in_specs.append(pl.BlockSpec(memory_space=pl.ANY))
        args.append(gram)
        aliases = {len(args): 0}
        body = kernel

        def kernel(*refs):
            body(*refs[:9], refs[-1])
    size = (n_direct + n_mirror) * 4 * BS * BS
    return call(
        kernel, (n_direct + n_mirror,), in_specs, pl.BlockSpec((2 * BS, 2 * BS), out_map),
        jax.ShapeDtypeStruct((dim, dim), BF16), idx, args, size * 64, size * 4, aliases=aliases,
    )


def solution(mesh):
    n_y = mesh.shape['fsdp']
    n_tp = mesh.shape['tp']
    mat_spec = P('stage', 'fsdp', 'tp')
    scalar_spec = P()
    pair_c = [(t, t ^ 1) for t in range(n_tp)]
    pair_x = [(t, t ^ 2) for t in range(n_tp)]
    pair_y = [(t, t ^ 1) for t in range(n_y)]

    def local_step(weight, momentum, gradient, learn_rate, mom_coef, weight_decay):
        row_dim = weight.shape[1] * n_y
        dim = weight.shape[2] * n_tp
        n_chunks = dim // (2 * BS)
        units = [(q, 0, q + 1) for q in range(n_chunks - 1)] + [(n_chunks - 1, 0, n_chunks // 2), (n_chunks - 1, n_chunks // 2, n_chunks)]
        tp = lax.axis_index('tp')
        y_pos = lax.axis_index('fsdp')
        core = lax.rem(tp, 2)
        x_pos = tp // 2
        table = []
        for q in range(n_chunks):
            table += [2 * q + core, 2 * q + 1 - core]
        table += [core, jnp.zeros_like(core), x_pos, y_pos, 2 * x_pos + y_pos, 2 * x_pos + 1 - y_pos]
        table += [2 * tp, 2 * tp + 1, 2 * tp + core, 2 * tp + 1 - core]
        order = Order(jnp.stack(table).astype(jnp.int32))

        def pair_sum(value):
            for axis, pairs in (('tp', pair_c), ('tp', pair_x), ('fsdp', pair_y)):
                value = value + lax.ppermute(value, axis, pairs)
            return value

        grad_full = gradient[0].astype(F32)
        nesterov = grad_full + mom_coef * (mom_coef * momentum[0] + grad_full)
        norm_val = jnp.sqrt(pair_sum(jnp.sum(nesterov * nesterov).reshape(1)))
        x_own = start_x(momentum[0], gradient[0], jnp.stack([mom_coef, norm_val[0] + NORM_EPS]))
        mom_old, grad_old, x_own = lax.optimization_barrier((momentum[0], gradient[0], x_own))
        mom_new = mom_coef * mom_old + grad_old.astype(F32)
        x_all = lax.all_gather(x_own, 'tp', axis=0, tiled=True)
        x_all = x_all.reshape(dim // BS, BS, x_all.shape[-1])
        pieces = [(x_all, at) for at in range(2 * n_chunks)]

        class Unit:
            def __init__(self, pieces, num):
                self.where = units[num]
                self.keep, send = gram_unit(order.idx, pieces, *self.where)
                order.after(self.keep)
                self.got = lax.ppermute(send, 'fsdp', pair_y)

            def reduce(self, wait=True):
                mine = (self.keep + self.got).astype(BF16)
                self.parts = [mine, lax.ppermute(mine, 'fsdp', pair_y), lax.ppermute(mine, 'tp', pair_x)]
                if wait:
                    order.after(mine)

            def spread(self, wait=True):
                self.parts.append(lax.ppermute(self.parts[1], 'tp', pair_x))
                self.parts += [lax.ppermute(part, 'tp', pair_c) for part in self.parts]
                if wait:
                    order.after(self.parts[1], self.parts[2])

            def place(self, gram):
                gram = unpack(order.idx, gram, self.parts, dim, *self.where)
                return gram

        last = n_chunks - 1
        flying = []
        for num in range(len(units)):
            flying.append(Unit(pieces, num))
            if num >= 2:
                flying[num - 2].reduce()
        for num in range(len(units)):
            if num > last - 1:
                flying[num].reduce(wait=False)
            flying[num].spread(wait=False)
        gram = None
        for unit in flying:
            gram = unit.place(gram)
        for _ in range(NS_STEPS - 1):
            flying, new_pieces = [], []
            poly = poly_rows(order.idx, gram, 0)
            for q in range(n_chunks):
                order.after(poly)
                mine = update_chunk(order.idx, poly, pieces, q)
                order.after(mine)
                new_pieces += [(mine, ZERO), (lax.ppermute(mine, 'tp', pair_c), ZERO)]
                if q >= 1 and q < last:
                    flying[q - 1].reduce()
                if q < last:
                    poly = poly_rows(order.idx, gram, 2 * (q + 1))
                    order.after(poly)
                    if q >= 1:
                        flying[q - 1].spread()
                    flying.append(Unit(new_pieces, q))
            flying.append(Unit(new_pieces, last))
            flying[last - 1].reduce()
            flying.append(Unit(new_pieces, last + 1))
            flying[last - 1].spread(wait=False)
            gram = None
            for num in range(last - 1):
                gram = flying[num].place(gram)
            for unit in flying[last:]:
                unit.reduce(wait=False)
                unit.spread(wait=False)
            for unit in flying[last - 1:]:
                gram = unit.place(gram)
            pieces = new_pieces
        step_scale = learn_rate * 0.2 * math.sqrt(row_dim)
        scalars = jnp.stack([1.0 - learn_rate * weight_decay, step_scale])
        new_weight = None
        for half in range(2):
            poly = poly_rows(order.idx, gram, MINE + half)
            new_weight = finish(order.idx, scalars, poly, weight[0], pieces, half, new_weight)
        return new_weight[None], mom_new[None]


    return jax.shard_map(local_step, mesh=mesh, in_specs=(mat_spec,) * 3 + (scalar_spec,) * 3, out_specs=(mat_spec, mat_spec), check_vma=False)
```
